32 devices in a mesh: rep: 4 (over x, y), dp: 8 (over z, core).
Axes of the slice: x: 2, y: 2, z: 4, core: 2. Of those that a mesh axis runs over, the one named last changes fastest.
Arguments:
- x: bfloat16 [32, 1024, 512], P(('rep', 'dp')), parts along dimension 0
- dy: bfloat16 [32, 1024, 512], P(('rep', 'dp')), parts along dimension 0
- w_gate: bfloat16 [2, 512, 8192], P(None, 'dp')
- w_up: bfloat16 [2, 512, 8192], P(None, 'dp')
- w_down: bfloat16 [2, 8192, 512], P(None, 'dp')
- m_w_gate: float32 [2, 512, 8192], P(None, 'dp')
- m_w_up: float32 [2, 512, 8192], P(None, 'dp')
- m_w_down: float32 [2, 8192, 512], P(None, 'dp')
- v_w_gate: float32 [2, 512, 8192], P(None, 'dp')
- v_w_up: float32 [2, 512, 8192], P(None, 'dp')
- v_w_down: float32 [2, 8192, 512], P(None, 'dp')
Outputs:
- output 1: bfloat16 [8, 512, 8192], P('rep', 'dp'), parts along dimension 0
- output 2: bfloat16 [8, 512, 8192], P('rep', 'dp'), parts along dimension 0
- output 3: bfloat16 [8, 8192, 512], P('rep', 'dp'), parts along dimension 0
- output 4: float32 [8, 512, 8192], P('rep', 'dp'), parts along dimension 0
- output 5: float32 [8, 512, 8192], P('rep', 'dp'), parts along dimension 0
- output 6: float32 [8, 8192, 512], P('rep', 'dp'), parts along dimension 0
- output 7: float32 [8, 512, 8192], P('rep', 'dp'), parts along dimension 0
- output 8: float32 [8, 512, 8192], P('rep', 'dp'), parts along dimension 0
- output 9: float32 [8, 8192, 512], P('rep', 'dp'), parts along dimension 0
There are 4 independent parts. The reference program is written for one: setup_inputs(seed, part) draws one part's arguments, and reference() takes and returns one part's arrays. A program takes and returns all parts, laid end to end along the dimension named above; an argument that names none is the same for every part.
All inputs are finite; a program needn't handle non-finite values.
Results may differ from the reference program's by a relative error of at most 0.022.
Values are sent between devices in bfloat16 or wider.
A program may use at most 2 GiB of HBM per device.

```python
import jax
import jax.numpy as jnp
from jax import lax

SEQUENCES = 8
TOKENS = 1024
D = 512
FF = 8192
LAYERS = 2
NAMES = ("w_gate", "w_up", "w_down")
SHAPES = {"w_gate": (LAYERS, D, FF), "w_up": (LAYERS, D, FF), "w_down": (LAYERS, FF, D)}


def bump(key, n, height):
    away = (jnp.arange(n, dtype=jnp.int32) - jax.random.randint(key, (), 0, n, jnp.int32)) % n
    return jnp.where(away < n // 8, height, 1.0)


def together(key, own, strength):
    shared = jax.random.normal(key, own.shape[1:], jnp.float32)
    return (own + strength * shared) * lax.rsqrt(1 + strength * strength)


def setup_inputs(seed: int = 0, part: int = 0) -> dict:
    kx, kdy, ka, kb, kz, kf, kh, kl, *keys = jax.random.split(jax.random.key(seed), 8 + 3 * len(NAMES))
    kx, kdy, ka, kb = (jax.random.fold_in(k, part) for k in (kx, kdy, ka, kb))
    kw, km, kv = (keys[i::3] for i in range(3))
    shape = (SEQUENCES, TOKENS, D)
    much_x, much_dy = jax.random.uniform(kz, (2,), jnp.float32, 0.0, 1.0)
    loud = 2.0 ** jax.random.uniform(jax.random.fold_in(kz, 1), (), jnp.float32, -1.0, 2.0)
    layers = 2.0 ** jax.random.uniform(kl, (LAYERS, 1, 1), jnp.float32, -1.0, 1.0)
    x = together(ka, jax.random.normal(kx, shape, jnp.float32), much_x) * bump(kf, D, 4.0)
    dy = together(kb, jax.random.normal(kdy, shape, jnp.float32), much_dy)
    drawn = {"x": x.astype(jnp.bfloat16), "dy": (loud * dy * (SEQUENCES * TOKENS) ** -0.5).astype(jnp.bfloat16)}
    for key, name in zip(kw, NAMES, strict=True):
        w = jax.random.normal(key, SHAPES[name], jnp.float32) * SHAPES[name][1] ** -0.5
        drawn[name] = (w * {"w_gate": 1.0, "w_up": bump(kh, FF, 4.0), "w_down": layers}[name]).astype(jnp.bfloat16)
    for key, name in zip(km, NAMES, strict=True):
        drawn[f"m_{name}"] = 0.1 * jax.random.normal(key, SHAPES[name], jnp.float32)
    for key, name in zip(kv, NAMES, strict=True):
        drawn[f"v_{name}"] = jax.random.uniform(key, SHAPES[name], jnp.float32, 0.005, 0.015)
    return drawn


def matmul(a, w):
    return jnp.dot(a, w, preferred_element_type=jnp.float32).astype(jnp.bfloat16)


def normed(h):
    wide = h.astype(jnp.float32)
    scale = lax.rsqrt(jnp.mean(wide**2, -1, keepdims=True) + 1e-6)
    return (wide * scale).astype(jnp.bfloat16)


def layer(h, w):
    a = normed(h)
    gate = jnp.dot(a, w["w_gate"], preferred_element_type=jnp.float32)
    up = jnp.dot(a, w["w_up"], preferred_element_type=jnp.float32)
    return h + matmul((jax.nn.silu(gate) * up).astype(jnp.bfloat16), w["w_down"])


def adamw(w, m, v, g):
    m = 0.9 * m + 0.1 * g
    v = 0.95 * v + 0.05 * g * g
    step = m * lax.rsqrt(v + 1e-8) + 0.1 * w
    return (w - 0.02 * step).astype(jnp.bfloat16), m, v


def clipped(gradients, sum_of_squares, count):
    factor = jnp.minimum(1.0, 0.5 * lax.rsqrt(sum_of_squares / count + 1e-30))
    return [g * factor for g in gradients]


def stack(weights, h):
    return lax.scan(lambda h, w: (layer(h, w), None), h, weights)[0]


def reference(x, dy, w_gate, w_up, w_down, m_w_gate, m_w_up, m_w_down, v_w_gate, v_w_up, v_w_down):
    weights = dict(zip(NAMES, (w_gate, w_up, w_down), strict=True))

    def take(so_far, sequence):
        h, by_y = sequence
        _, back = jax.vjp(lambda w: stack(w, h), weights)
        return jax.tree.map(lambda total, term: total + term.astype(jnp.float32), so_far, back(by_y)[0]), None

    none_yet = {name: jnp.zeros(w.shape, jnp.float32) for name, w in weights.items()}
    by_weights, _ = lax.scan(take, none_yet, (x, dy))
    gradients = [by_weights[name].astype(jnp.bfloat16).astype(jnp.float32) for name in NAMES]
    gradients = clipped(gradients, sum(jnp.sum(g * g) for g in gradients), sum(g.size for g in gradients))
    new = [
        adamw(w.astype(jnp.float32), m, v, g)
        for w, m, v, g in zip((w_gate, w_up, w_down), (m_w_gate, m_w_up, m_w_down), (v_w_gate, v_w_up, v_w_down), gradients, strict=True)
    ]
    return tuple(one[which] for which in range(3) for one in new)
```

```python
import jax
import jax.numpy as jnp
from jax import lax
from jax.experimental import pallas as pl
from jax.experimental.pallas import tpu as pltpu
from jax.sharding import Mesh, PartitionSpec as P

ANY = pl.ANY
REPS, ZS, CORES = 4, 4, 2


PARTS = ((0, 0), (1, 0), (2, 0), (2, 1))


def gather_kernel(*refs):
    n = len(PARTS)
    weights, outs, held = refs[:3], refs[3 : 3 + n], refs[3 + n : 3 + 2 * n]
    ld, st, ps, pr, sa, ra, sb, rb, sc, rc = refs[3 + 2 * n :]
    ins = [weights[which].at[layer] for which, layer in PARTS]
    r, z, c = (lax.axis_index(axis) for axis in ("rep", "z", "core"))
    d = z * 2 + c
    partner = d + 1 - 2 * c
    barrier = pltpu.get_barrier_semaphore()

    def at(rep, dp):
        return (rep, dp // 2, dp % 2)

    def up(k):
        return lax.rem(z + k, ZS) * 2 + c

    def col(k):
        return lax.rem(r + k, REPS)

    near = [at(r, partner)] + [at(r, up(k)) for k in (1, 2, 3)] + [at(col(k), d) for k in (1, 2, 3)]
    loads = [pltpu.make_async_copy(i, h, ld.at[m]) for m, (i, h) in enumerate(zip(ins, held))]
    for one in loads:
        one.start()
    for one in near:
        pl.semaphore_signal(barrier, inc=1, device_id=one, device_id_type=pl.DeviceIdType.MESH)
    pl.semaphore_wait(barrier, len(near))

    def quarter(ref, m, owner, q):
        rows = ref.shape[0] // (8 if owner is not None else 1)
        first = 0 if owner is None else owner * rows
        if PARTS[m][0] < 2:
            wide = ref.shape[1] // REPS
            return ref.at[pl.ds(first, rows), pl.ds(pl.multiple_of(q * wide, wide), wide)]
        deep = rows // REPS
        return ref.at[pl.ds(pl.multiple_of(first + q * deep, deep), deep), :]

    def shard(ref, owner):
        rows = ref.shape[0] // 8
        return ref.at[pl.ds(pl.multiple_of(owner * rows, rows), rows), :]

    def remote(src, dst, s, t, to):
        return pltpu.make_async_remote_copy(src_ref=src, dst_ref=dst, send_sem=s, recv_sem=t, device_id=to, device_id_type=pl.DeviceIdType.MESH)

    started = []
    own = []
    for m in range(n):
        loads[m].wait()
        for k in (1, 3, 2):
            one = remote(quarter(held[m], m, None, r), quarter(outs[m], m, d, r), sa.at[m, k - 1], ra.at[m, k - 1], at(r, up(k)))
            one.start()
            started.append(one)
        one = remote(held[m], shard(outs[m], d), ps.at[m], pr.at[m], at(r, partner))
        one.start()
        started.append(one)
        mine = pltpu.make_async_copy(held[m], shard(outs[m], d), st.at[m])
        mine.start()
        own.append(mine)
    for m in range(n):
        for k in (1, 3, 2):
            src = lax.rem(z + ZS - k, ZS) * 2 + c
            piece = quarter(outs[m], m, src, r)
            remote(quarter(held[m], m, None, r), piece, sa.at[m, k - 1], ra.at[m, k - 1], at(r, up(k))).wait_recv()
            for j in (3, 1, 2):
                one = remote(piece, piece, sb.at[m, k - 1, j - 1], rb.at[m, k - 1, j - 1], at(col(j), d))
                one.start()
                started.append(one)
    for m in range(n):
        for k in (1, 3, 2):
            src = lax.rem(z + ZS - k, ZS) * 2 + c
            for j in (3, 1, 2):
                piece = quarter(outs[m], m, src, lax.rem(r + REPS - j, REPS))
                remote(piece, piece, sb.at[m, k - 1, j - 1], rb.at[m, k - 1, j - 1], at(col(j), d)).wait_recv()
            one = remote(shard(outs[m], src), shard(outs[m], src), sc.at[m, k - 1], rc.at[m, k - 1], at(r, partner))
            one.start()
            started.append(one)
    for m in range(n):
        remote(held[m], shard(outs[m], partner), ps.at[m], pr.at[m], at(r, partner)).wait_recv()
        for k in (1, 3, 2):
            src = lax.rem(z + ZS - k, ZS) * 2 + 1 - c
            remote(shard(outs[m], src), shard(outs[m], src), sc.at[m, k - 1], rc.at[m, k - 1], at(r, partner)).wait_recv()
    for one in own:
        one.wait()
    for one in started:
        one.wait_send()


def gather(weights, collective_id):
    dma = pltpu.SemaphoreType.DMA
    n, shards = len(PARTS), [weights[which].shape[1:] for which, _ in PARTS]
    return pl.pallas_call(
        gather_kernel,
        out_shape=[jax.ShapeDtypeStruct((ZS * CORES * rows, columns), jnp.bfloat16) for rows, columns in shards],
        in_specs=[pl.BlockSpec(memory_space=ANY)] * 3,
        out_specs=[pl.BlockSpec(memory_space=ANY)] * n,
        scratch_shapes=[pltpu.VMEM(shape, jnp.bfloat16) for shape in shards]
        + [dma((n,))] * 4
        + [dma((n, 3))] * 2
        + [dma((n, 3, 3))] * 2
        + [dma((n, 3))] * 2,
        compiler_params=pltpu.CompilerParams(collective_id=collective_id, has_side_effects=True),
        name="gather",
    )(*weights)


def matmul(a, w):
    return jnp.dot(a, w, preferred_element_type=jnp.float32).astype(jnp.bfloat16)


def over_tokens(a, b):
    return lax.dot_general(a, b, (((0,), (0,)), ((), ())), preferred_element_type=jnp.float32).astype(jnp.bfloat16)


def back_to(a, w):
    return lax.dot_general(a, w, (((1,), (1,)), ((), ())), preferred_element_type=jnp.float32).astype(jnp.bfloat16)


def normed(h):
    wide = h.astype(jnp.float32)
    scale = lax.rsqrt(jnp.mean(wide**2, -1, keepdims=True) + 1e-6)
    return (wide * scale).astype(jnp.bfloat16)


def gated(gate, up):
    return (jax.nn.silu(gate) * up).astype(jnp.bfloat16)


def projection_kernel(a, w_gate, w_up, gate, up, hidden):
    gate[...] = jnp.dot(a[...], w_gate[...], preferred_element_type=jnp.float32)
    up[...] = jnp.dot(a[...], w_up[...], preferred_element_type=jnp.float32)
    hidden[...] = gated(gate[...], up[...])


def projections(a, w):
    (tokens, d), ff, tile = a.shape, w[0].shape[1], 512
    wide = pl.BlockSpec((tokens, tile), lambda i: (0, i))
    return pl.pallas_call(
        projection_kernel,
        grid=(ff // tile,),
        out_shape=[jax.ShapeDtypeStruct((tokens, ff), kind) for kind in (jnp.float32, jnp.float32, jnp.bfloat16)],
        in_specs=[pl.BlockSpec((tokens, d), lambda i: (0, 0))] + [pl.BlockSpec((d, tile), lambda i: (0, i))] * 2,
        out_specs=[wide] * 3,
        cost_estimate=pl.CostEstimate(flops=4 * tokens * d * ff, bytes_accessed=10 * tokens * ff + 4 * d * ff, transcendentals=tokens * ff),
        name="projections",
    )(a, w[0], w[1])


def input_kernel(by_gate, by_up, w_gate, w_up, token, by_a, of_gate, of_up):
    @pl.when(pl.program_id(0) == 0)
    def _():
        of_gate[...] = jnp.zeros_like(of_gate)
        of_up[...] = jnp.zeros_like(of_up)

    across = (((1,), (1,)), ((), ()))
    of_gate[...] += lax.dot_general(by_gate[...], w_gate[...], across, preferred_element_type=jnp.float32)
    of_up[...] += lax.dot_general(by_up[...], w_up[...], across, preferred_element_type=jnp.float32)

    @pl.when(pl.program_id(0) == pl.num_programs(0) - 1)
    def _():
        wide = of_gate[...].astype(jnp.bfloat16).astype(jnp.float32) + of_up[...].astype(jnp.bfloat16).astype(jnp.float32)
        by_a[...] = wide.astype(jnp.bfloat16)


def back_to_input(by_gate, by_up, w, token):
    (tokens, ff), d, tile = by_gate.shape, w[0].shape[0], 512
    return pl.pallas_call(
        input_kernel,
        grid=(ff // tile,),
        out_shape=jax.ShapeDtypeStruct((tokens, d), jnp.bfloat16),
        in_specs=[pl.BlockSpec((tokens, tile), lambda i: (0, i))] * 2
        + [pl.BlockSpec((d, tile), lambda i: (0, i))] * 2
        + [pl.BlockSpec(memory_space=ANY)],
        out_specs=pl.BlockSpec((tokens, d), lambda i: (0, 0)),
        scratch_shapes=[pltpu.VMEM((tokens, d), jnp.float32)] * 2,
        cost_estimate=pl.CostEstimate(flops=4 * tokens * d * ff, bytes_accessed=4 * ff * (tokens + d), transcendentals=0),
        name="back_to_input",
    )(by_gate, by_up, w[0], w[1], token)


def total_kernel(x, out, slots, send, recv):
    r, z, c = (lax.axis_index(axis) for axis in ("rep", "z", "core"))
    n, d = ZS * CORES, z * CORES + c
    barrier = pltpu.get_barrier_semaphore()

    def to(k):
        other = lax.rem(d + k, n)
        return (r, other // CORES, other % CORES)

    for k in range(1, n):
        pl.semaphore_signal(barrier, inc=1, device_id=to(k), device_id_type=pl.DeviceIdType.MESH)
    pl.semaphore_wait(barrier, n - 1)
    copies = [
        pltpu.make_async_remote_copy(
            src_ref=x, dst_ref=slots.at[d], send_sem=send.at[k - 1], recv_sem=recv.at[k - 1], device_id=to(k), device_id_type=pl.DeviceIdType.MESH
        )
        for k in range(1, n)
    ]
    for one in copies:
        one.start()
    slots[d] = x[...]
    for one in copies:
        one.wait()
    out[...] = sum(slots[i] for i in range(n))


def total(x, collective_id):
    shape = (8, 128)
    return pl.pallas_call(
        total_kernel,
        out_shape=jax.ShapeDtypeStruct(shape, jnp.float32),
        in_specs=[pl.BlockSpec(memory_space=pltpu.VMEM)],
        out_specs=pl.BlockSpec(memory_space=pltpu.VMEM),
        scratch_shapes=[pltpu.VMEM((ZS * CORES,) + shape, jnp.float32)] + [pltpu.SemaphoreType.DMA((ZS * CORES - 1,))] * 2,
        compiler_params=pltpu.CompilerParams(collective_id=collective_id, has_side_effects=True),
        name="total",
    )(jnp.broadcast_to(x, shape))[0, 0]


def after_kernel(x, token, y):
    y[...] = x[...]


def after(x, token):
    return pl.pallas_call(
        after_kernel,
        out_shape=jax.ShapeDtypeStruct(x.shape, x.dtype),
        in_specs=[pl.BlockSpec(memory_space=pltpu.VMEM), pl.BlockSpec(memory_space=ANY)],
        out_specs=pl.BlockSpec(memory_space=pltpu.VMEM),
        name="after",
    )(x, token)


def adamw(w, m, v, g):
    m = 0.9 * m + 0.1 * g
    v = 0.95 * v + 0.05 * g * g
    step = m * lax.rsqrt(v + 1e-8) + 0.1 * w
    return (w - 0.02 * step).astype(jnp.bfloat16), m, v


def solution(mesh):
    cells = Mesh(mesh.devices.reshape(REPS, ZS, CORES), ("rep", "z", "core"))
    everyone, line = ("rep", "z", "core"), ("z", "core")

    def backward(h, by_h, w, kept, deeper):
        a, from_a = jax.vjp(normed, h)
        gate, up, hidden = kept(a, w)
        down = over_tokens(hidden, by_h)
        scattered = [lax.psum_scatter(down, line, scatter_dimension=0, tiled=True)]
        by_h = after(by_h, down)
        by_gate, by_up = (by.astype(jnp.bfloat16) for by in jax.vjp(gated, gate, up)[1](back_to(by_h, w[2])))
        both = jnp.concatenate([over_tokens(a, by_gate), over_tokens(a, by_up)], axis=1)
        summed = lax.psum_scatter(both, line, scatter_dimension=0, tiled=True)
        by_x = from_a(back_to_input(by_gate, by_up, w, both))[0] + by_h if deeper else None
        return jnp.split(summed, 2, axis=1) + scattered, by_x

    def step(x, dy, *arrays):
        weights, m, v = (arrays[i : i + 3] for i in (0, 3, 6))
        *first, last_down = gather(weights, 3)
        second = [lax.all_gather(w[1], line, axis=0, tiled=True) for w in weights[:2]] + [last_down]
        x, dy = x[0], dy[0]
        lowest = projections(normed(x), first)
        h = x + matmul(lowest[2], first[2])
        late, by_h = backward(h, dy, second, projections, True)
        early, _ = backward(x, by_h, first, lambda a, w: lowest, False)
        early[2] = after(early[2], late[0])
        squares = total(sum(jnp.sum(g.astype(jnp.float32) ** 2) for g in late + early), 4)
        mine = [jnp.stack([e, l]).astype(jnp.float32) for e, l in zip(early, late)]
        count = sum(g.size for g in mine) * ZS * CORES
        factor = jnp.minimum(1.0, 0.5 * lax.rsqrt(squares / count + 1e-30))
        new = [adamw(w.astype(jnp.float32), m, v, g * factor) for w, m, v, g in zip(weights, m, v, mine, strict=True)]
        return tuple(one[which] for which in range(3) for one in new)

    states, cut = P(everyone, None, None), P(None, line, None)
    return jax.shard_map(
        step,
        mesh=cells,
        in_specs=(states, states) + (cut,) * 9,
        out_specs=(P("rep", line, None),) * 9,
        check_vma=False,
    )
```
